32 devices in a mesh: groups: 2 (over x), ctx: 16 (over z, y, core).
Axes of the slice: x: 2, y: 2, z: 4, core: 2. Of those that a mesh axis runs over, the one named last changes fastest.
Arguments:
- queries: bfloat16 [3072, 16, 128], P(('groups', 'ctx')), parts along dimension 0, may hold values from -12 to 12
- keys: bfloat16 [3072, 4, 128], P(('groups', 'ctx')), parts along dimension 0, may hold values from -5 to 5
- values: bfloat16 [3072, 4, 128], P(('groups', 'ctx')), parts along dimension 0, may hold values from -6 to 6
- positions: int32 [3072], P(('groups', 'ctx')), parts along dimension 0, may hold values from 0 to 1535, as said below
Outputs:
- attended: bfloat16 [3072, 16, 128], P(('groups', 'ctx')), parts along dimension 0
The draws below stay inside these ranges and needn't reach their ends.
There are 2 independent parts, one for each index of `groups`. The reference program is written for one: setup_inputs(seed, part) draws one part's arguments, and reference() takes and returns one part's arrays. A program takes and returns all parts, laid end to end along the dimension named above; each array names one. Nothing has to cross between parts.
Inputs may be any that keep to these rules, and one draw needn't show every extreme that they name: A permutation of 0 to 1535 in which the 96 rows of each device along ctx hold the positions c, c + 16, c + 32 and so on in that order, for one offset c a device, the offsets of the devices being a permutation of 0 to 15.
All inputs are finite; a program needn't handle non-finite values.
Results may differ from the reference program's by a relative error of at most 0.0091.
Values may be sent and summed in bfloat16 or wider, within the bound.
A program may use at most 64 MiB of HBM per device.

```python
import math
import jax
import jax.numpy as jnp
from jax import lax

H = 16
KVH = 4
HD = 128
TOK_DEV = 96
SEQ = 1536
STRIDE = 16


def draw_common(key):
    base = jax.random.fold_in(key, 11)
    first_key, second_key = jax.random.split(base, 2)
    query_draw = jnp.clip(jax.random.normal(first_key, (SEQ, H, HD), jnp.float32) * 2.5, -12.0, 12.0)
    key_draw = jnp.clip(jax.random.normal(second_key, (SEQ, KVH, HD), jnp.float32), -5.0, 5.0)
    return (query_draw, key_draw)


def draw_queries(key, part):
    return draw_common(key)[0].astype(jnp.bfloat16)


def draw_keys(key, part):
    return draw_common(key)[1].astype(jnp.bfloat16)


def draw_positions(key, part):
    offsets = jax.random.permutation(jax.random.fold_in(key, 3), STRIDE)
    steps_along = jnp.arange(TOK_DEV, dtype=jnp.int32)
    placed = steps_along[None, :] * STRIDE + offsets.astype(jnp.int32)[:, None]
    return placed.reshape(-1).astype(jnp.int32)


def levels(stream_key, dims, pieces, low, largest):
    factor_of, own = 1.0, jax.random.fold_in(stream_key, 6)
    for dim, blocks in pieces:
        steps = jnp.exp(jax.random.uniform(jax.random.fold_in(own, dim), (blocks,), jnp.float32, low / len(pieces), largest / len(pieces)))
        factor_of = factor_of * jnp.repeat(steps, dims[dim] // blocks).reshape([-1 if axis == dim else 1 for axis in range(len(dims))])
    return factor_of


def scatter_about(stream_key, extent, width, limit, cuts=(), kind=jnp.bfloat16):
    drawn = width * jax.random.normal(stream_key, extent, jnp.float32)
    if cuts:
        drawn = drawn * levels(stream_key, extent, cuts, -0.22, 0.18)
    return jnp.clip(drawn, -limit, limit).astype(kind)


def setup_inputs(seed: int = 0, part: int = 0) -> dict:
    key_of = jax.random.split(jax.random.key(seed), 5)
    part_splits = jax.random.split(jax.random.fold_in(key_of[4], part), 5)
    return {
        "queries": draw_queries(jax.random.fold_in(jax.random.fold_in(key_of[4], part), 71), part),
        "keys": draw_keys(jax.random.fold_in(jax.random.fold_in(key_of[4], part), 71), part),
        "values": scatter_about(part_splits[2], (SEQ, KVH, HD), 1.0, 6.0, ((0, 16),)),
        "positions": draw_positions(jax.random.fold_in(jax.random.fold_in(key_of[4], part), 71), part),
    }


def rotate(tensor, places):
    half_size = tensor.shape[-1] // 2
    inverse = jnp.power(jnp.float32(1000000.0), -jnp.arange(half_size, dtype=jnp.float32) * 2.0 / tensor.shape[-1])
    angles = places.astype(jnp.float32)[:, None] * inverse[None, :]
    cosine = jnp.cos(angles)[:, None, :]
    sines = jnp.sin(angles)[:, None, :]
    floats = tensor.astype(jnp.float32)
    leading = floats[..., :half_size]
    trailing = floats[..., half_size:]
    return jnp.concatenate([leading * cosine - trailing * sines, trailing * cosine + leading * sines], -1).astype(jnp.bfloat16)

def reference(queries, keys, values, positions):
    q_rot = rotate(queries, positions)
    k_rot = rotate(keys, positions)
    scaling = 1.0 / math.sqrt(HD)
    rows_block = math.gcd(SEQ, 512)
    grouped = q_rot.reshape(SEQ // rows_block, rows_block, KVH, H // KVH, HD)
    places = positions.reshape(SEQ // rows_block, rows_block)
    key_float = k_rot.astype(jnp.float32)
    value_float = values.astype(jnp.float32)

    def one_block(inputs):
        query_part, query_places = inputs
        scores = jnp.einsum('bkgd,skd->kgbs', query_part.astype(jnp.float32), key_float) * scaling
        allowed = query_places[:, None] >= positions[None, :]
        scores = jnp.where(allowed[None, None], scores, -jnp.inf)
        maxima = lax.optimization_barrier(jnp.max(scores, axis=-1, keepdims=True))
        weights = jnp.exp(scores - maxima)
        totals = lax.optimization_barrier(jnp.sum(weights, axis=-1))
        rounded = lax.optimization_barrier(weights.astype(jnp.bfloat16)).astype(jnp.float32)
        output = jnp.einsum('kgbs,skd->kgbd', rounded, value_float) / totals[..., None]
        return output.transpose(2, 0, 1, 3).reshape(rows_block, H, HD).astype(jnp.bfloat16)
    outputs = lax.map(one_block, (grouped, places))
    return outputs.reshape(SEQ, H, HD)
```

```python
import functools
import math

import jax
import jax.numpy as jnp
import numpy as np
from jax import lax
from jax.experimental import pallas as pl
from jax.experimental.pallas import tpu as pltpu
from jax.sharding import PartitionSpec as P

UNIT = 16
PIECES = 2
PLANE = 4


def rotary_tables(tokens, head_size, stride):
    half = head_size // 2
    inverse = 1000000.0 ** (-2.0 * np.arange(half) / head_size)
    angles = (stride * np.arange(tokens))[:, None] * inverse[None, :]
    wide = lambda x: np.concatenate([x, x], -1)
    return np.concatenate(
        [wide(np.cos(angles)), wide(np.sin(angles)), wide(np.tile(inverse, (8, 1)))]
    ).astype(np.float32)


def attend(
    n, kv_heads, per_group, tokens,
    place_ref, q_ref, k_ref, v_ref, table_ref, out_ref,
    gathered, q_rot, wide, small, m_ref, l_ref, acc_ref,
    recv_sem, send_sem,
):
    head_size = q_ref.shape[-1]
    heads = kv_heads * per_group
    rows = n // PLANE
    me = lax.axis_index("ctx")
    core = me % 2
    column = me // 2 % 2
    z = me // PLANE
    units = tokens // UNIT
    tile = 2 * UNIT
    tiles = tokens // tile
    per_piece = kv_heads // PIECES
    lanes = per_group * tile
    factor = math.log2(math.e) / math.sqrt(head_size)

    def device(row, col, cr):
        return row * PLANE + col * 2 + cr

    barrier = pltpu.get_barrier_semaphore()
    across = device(z, 1 - column, core)
    mate = device(z, column, 1 - core)
    below = me - PLANE
    above = me + PLANE

    def greet(target):
        pl.semaphore_signal(barrier, inc=1, device_id={"ctx": target})

    greet(across)
    greet(mate)

    @pl.when(z > 0)
    def _():
        greet(below)

    @pl.when(z < rows - 1)
    def _():
        greet(above)

    offset = place_ref[0].astype(jnp.float32)
    start = table_ref[2 * tokens : 2 * tokens + 8, :] * offset
    c0, s0 = jnp.cos(start)[:1], jnp.sin(start)[:1]
    ct, st = table_ref[:tokens, :], table_ref[tokens : 2 * tokens, :]
    lane = lax.broadcasted_iota(jnp.int32, (tokens, head_size), 1)
    cosine = ct * c0 - st * s0
    sine = st * c0 + ct * s0
    sine = jnp.where(lane < head_size // 2, -sine, sine)

    def rotated(x):
        return (x * cosine + pltpu.roll(x, head_size // 2, 1) * sine).astype(jnp.bfloat16)

    small[0] = k_ref[...].astype(jnp.float32)
    small[1] = v_ref[...].astype(jnp.float32)
    for h in range(kv_heads):
        p, at = h // per_piece, h % per_piece * 2 * units
        k = rotated(small[0, pl.ds(h, tokens, stride=kv_heads), :])
        gathered[p, at : at + units, me] = k.reshape(units, UNIT, head_size)
        v = small[1, pl.ds(h, tokens, stride=kv_heads), :].astype(jnp.bfloat16)
        gathered[p, at + units : at + 2 * units, me] = v.reshape(units, UNIT, head_size)
    own = jnp.full((UNIT, head_size), offset, jnp.float32)
    for p in range(PIECES):
        gathered[p, 2 * units * per_piece, me] = own.astype(jnp.bfloat16)

    def copy(slot, p, target, kind):
        return pltpu.make_async_remote_copy(
            src_ref=gathered.at[p, :, slot],
            dst_ref=gathered.at[p, :, slot],
            send_sem=send_sem.at[kind, slot, p],
            recv_sem=recv_sem.at[slot, p],
            device_id={"ctx": target},
        )

    def arrived(slot, p):
        copy(slot, p, mate, 0).wait_recv()

    def share(slot, p):
        copy(slot, p, across, 1).start()
        copy(slot, p, mate, 2).start()

    pl.semaphore_wait(barrier, 2 + (z > 0).astype(jnp.int32) + (z < rows - 1).astype(jnp.int32))

    for p in range(PIECES):

        @pl.when(z > 0)
        def _():
            copy(me, p, below, 0).start()

        @pl.when(z < rows - 1)
        def _():
            copy(me, p, above, 3).start()

        share(me, p)

    wide[...] = q_ref[...].astype(jnp.float32)
    for h in range(heads):
        k, g = divmod(h, per_group)
        q = rotated(wide[pl.ds(h, tokens, stride=heads), :])
        for t in range(tiles):
            q_rot[k, t * lanes + g * tile : t * lanes + (g + 1) * tile] = q[t * tile : (t + 1) * tile]

    width = tiles * lanes
    m_ref[...] = jnp.full(m_ref.shape, -jnp.inf, jnp.float32)
    l_ref[...] = jnp.zeros(l_ref.shape, jnp.float32)
    acc_ref[...] = jnp.zeros(acc_ref.shape, jnp.float32)

    keys_tile = PLANE * tile
    key_row = lax.broadcasted_iota(jnp.int32, (keys_tile, lanes), 0)
    key_at = key_row // (PLANE * UNIT) * UNIT + key_row % UNIT
    query_at = lax.broadcasted_iota(jnp.int32, (keys_tile, lanes), 1) % tile

    def attend_plane(row):
        first = row * PLANE

        def head(k, p, at):
            theirs = gathered[p, 2 * units * per_piece, pl.ds(first, PLANE)]
            theirs = theirs.astype(jnp.float32).reshape(PLANE * UNIT, head_size)
            theirs = jnp.concatenate([theirs] * (tile // UNIT), 0)
            reach = key_at + (theirs > offset).astype(jnp.int32)
            allowed = reach <= query_at
            scores = []
            for t in range(tiles):
                keys = gathered[p, pl.ds(at + 2 * t, 2), pl.ds(first, PLANE)]
                keys = keys.reshape(keys_tile, head_size)
                s = lax.dot_general(
                    keys, q_rot[k, t * lanes :],
                    (((1,), (1,)), ((), ())), preferred_element_type=jnp.float32,
                )
                diagonal = jnp.where(allowed, s[:, :lanes], -jnp.inf)
                scores.append([diagonal] + [s[:, i * lanes : (i + 1) * lanes] for i in range(1, tiles - t)])
            old = m_ref[k]
            weights = [[] for _ in range(tiles)]
            shrinks = []
            for i in range(tiles):
                span = slice(i * lanes, (i + 1) * lanes)
                mine = [scores[t][i - t] for t in range(i + 1)]
                top = old[:, span]
                for s in mine:
                    top = jnp.maximum(top, jnp.max(s, axis=0, keepdims=True))
                shrink = jnp.exp2((old[:, span] - top) * factor)
                total = l_ref[k, :, span] * shrink
                for t in range(i + 1):
                    w = jnp.exp2((mine[t] - top) * factor)
                    total += jnp.sum(w, axis=0, keepdims=True)
                    weights[t].append(w.astype(jnp.bfloat16))
                m_ref[k, :, span] = top
                l_ref[k, :, span] = total
                shrinks.append(shrink)
            sums = [acc_ref[k, :, i * lanes : (i + 1) * lanes] * shrinks[i] for i in range(tiles)]
            for t in range(tiles):
                values = gathered[p, pl.ds(at + units + 2 * t, 2), pl.ds(first, PLANE)]
                values = values.reshape(keys_tile, head_size)
                w = jnp.concatenate(weights[t], 1)
                o = lax.dot_general(
                    values, w, (((0,), (0,)), ((), ())), preferred_element_type=jnp.float32
                )
                for i in range(t, tiles):
                    sums[i] += o[:, (i - t) * lanes : (i - t + 1) * lanes]
            for i in range(tiles):
                acc_ref[k, :, i * lanes : (i + 1) * lanes] = sums[i]

        for p in range(PIECES):
            for col in range(2):
                arrived(device(row, col, 1 - core), p)

            @pl.loop(0, per_piece)
            def _(i):
                head(p * per_piece + i, p, i * 2 * units)

    def either(step, do):
        @pl.when(z >= step)
        def _():
            do(z - step, False)

        @pl.when(z + step < rows)
        def _():
            do(z + step, True)

    def relay_column(step):
        for p in range(PIECES):

            def do(row, from_above):
                slot = device(row, column, core)
                arrived(slot, p)
                if from_above:

                    @pl.when(z > 0)
                    def _():
                        copy(slot, p, below, 0).start()
                else:

                    @pl.when(z < rows - 1)
                    def _():
                        copy(slot, p, above, 3).start()
                share(slot, p)

            either(step, do)

    def relay_across(row):
        for p in range(PIECES):
            slot = device(row, 1 - column, core)
            arrived(slot, p)
            copy(slot, p, mate, 2).start()

    def finish(row, from_above):
        relay_across(row)
        attend_plane(row)

    relay_column(1)
    relay_across(z)
    attend_plane(z)

    @pl.loop(1, rows)
    def _(step):
        @pl.when(step + 1 < rows)
        def _():
            relay_column(step + 1)

        either(step, finish)

    for k in range(kv_heads):
        o = (acc_ref[k] / l_ref[k]).T
        for t in range(tiles):
            for g in range(per_group):
                at = t * lanes + g * tile
                wide[pl.ds(t * tile * heads + k * per_group + g, tile, stride=heads), :] = o[at : at + tile]
    out_ref[...] = wide[...].astype(jnp.bfloat16)

    def sent(row, from_above):
        for p in range(PIECES):
            slot = device(row, column, core)
            if from_above:

                @pl.when(z > 0)
                def _():
                    copy(slot, p, below, 0).wait_send()
            else:

                @pl.when(z < rows - 1)
                def _():
                    copy(slot, p, above, 3).wait_send()
            copy(slot, p, across, 1).wait_send()
            copy(slot, p, mate, 2).wait_send()
            copy(device(row, 1 - column, core), p, mate, 2).wait_send()

    @pl.loop(1, rows)
    def _(step):
        either(step, sent)

    sent(z, False)
    for p in range(PIECES):

        @pl.when(z > 0)
        def _():
            copy(me, p, below, 0).wait_send()


def solution(mesh):
    n = mesh.shape["ctx"]

    def shards(queries, keys, values, positions):
        tokens, heads, head_size = queries.shape
        kv_heads = keys.shape[1]
        per_group = heads // kv_heads
        table = rotary_tables(tokens, head_size, n)
        tile = 2 * UNIT
        width = tokens * per_group
        blocks = 2 * (tokens // UNIT) * (kv_heads // PIECES) + 1
        vmem = pl.BlockSpec(memory_space=pltpu.VMEM)
        out = pl.pallas_call(
            functools.partial(attend, n, kv_heads, per_group, tokens),
            out_shape=jax.ShapeDtypeStruct((tokens * heads, head_size), jnp.bfloat16),
            in_specs=[pl.BlockSpec(memory_space=pltpu.SMEM)] + [vmem] * 4,
            out_specs=vmem,
            scratch_shapes=[
                pltpu.VMEM((PIECES, blocks, n, UNIT, head_size), jnp.bfloat16),
                pltpu.VMEM((kv_heads, width, head_size), jnp.bfloat16),
                pltpu.VMEM((tokens * heads, head_size), jnp.float32),
                pltpu.VMEM((2, tokens * kv_heads, head_size), jnp.float32),
                pltpu.VMEM((kv_heads, 1, width), jnp.float32),
                pltpu.VMEM((kv_heads, 1, width), jnp.float32),
                pltpu.VMEM((kv_heads, head_size, width), jnp.float32),
                pltpu.SemaphoreType.DMA((n, PIECES)),
                pltpu.SemaphoreType.DMA((4, n, PIECES)),
            ],
            compiler_params=pltpu.CompilerParams(
                collective_id=0, has_side_effects=True, vmem_limit_bytes=48 * 1024 * 1024
            ),
        )(
            positions,
            queries.reshape(tokens * heads, head_size),
            keys.reshape(tokens * kv_heads, head_size),
            values.reshape(tokens * kv_heads, head_size),
            table,
        )
        return out.reshape(tokens, heads, head_size)

    placed = (
        P(("groups", "ctx"), None, None),
        P(("groups", "ctx"), None, None),
        P(("groups", "ctx"), None, None),
        P(("groups", "ctx")),
    )
    return jax.shard_map(
        shards,
        mesh=mesh,
        in_specs=placed,
        out_specs=P(("groups", "ctx"), None, None),
        check_vma=False,
    )
```

```python
import functools
import math

import jax
import jax.numpy as jnp
import numpy as np
from jax import lax
from jax.experimental import pallas as pl
from jax.experimental.pallas import tpu as pltpu
from jax.sharding import PartitionSpec as P

UNIT = 16
PIECES = 4
PLANE = 4


def rotary_tables(tokens, head_size, stride):
    half = head_size // 2
    inverse = 1000000.0 ** (-2.0 * np.arange(half) / head_size)
    angles = (stride * np.arange(tokens))[:, None] * inverse[None, :]
    wide = lambda x: np.concatenate([x, x], -1)
    return np.concatenate(
        [wide(np.cos(angles)), wide(np.sin(angles)), wide(np.tile(inverse, (8, 1)))]
    ).astype(np.float32)


def attend(
    n, kv_heads, per_group, tokens,
    place_hbm, q_hbm, k_hbm, v_hbm, table_hbm, out_ref,
    gathered, q_rot, wide, small, m_ref, l_ref, acc_ref,
    place_ref, q_ref, k_ref, v_ref, table_ref,
    recv_sem, send_sem, load_sem,
):
    loads = [
        pltpu.make_async_copy(src, dst, load_sem.at[i])
        for i, (src, dst) in enumerate(
            [(place_hbm, place_ref), (table_hbm, table_ref), (k_hbm, k_ref), (v_hbm, v_ref), (q_hbm, q_ref)]
        )
    ]
    for load in loads:
        load.start()
    head_size = q_ref.shape[-1]
    heads = kv_heads * per_group
    rows = n // PLANE
    me = lax.axis_index("ctx")
    core = me % 2
    column = me // 2 % 2
    z = me // PLANE
    units = tokens // UNIT
    tile = 2 * UNIT
    tiles = tokens // tile
    per_piece = kv_heads // PIECES
    lanes = per_group * tile
    factor = math.log2(math.e) / math.sqrt(head_size)

    def device(row, col, cr):
        return row * PLANE + col * 2 + cr

    barrier = pltpu.get_barrier_semaphore()
    across = device(z, 1 - column, core)
    mate = device(z, column, 1 - core)
    below = me - PLANE
    above = me + PLANE

    def greet(target):
        pl.semaphore_signal(barrier, inc=1, device_id={"ctx": target})

    greet(across)
    greet(mate)

    @pl.when(z > 0)
    def _():
        greet(below)

    @pl.when(z < rows - 1)
    def _():
        greet(above)

    for load in loads[:2]:
        load.wait()
    offset = place_ref[0].astype(jnp.float32)
    start = table_ref[2 * tokens : 2 * tokens + 8, :] * offset
    c0, s0 = jnp.cos(start)[:1], jnp.sin(start)[:1]
    ct, st = table_ref[:tokens, :], table_ref[tokens : 2 * tokens, :]
    lane = lax.broadcasted_iota(jnp.int32, (tokens, head_size), 1)
    cosine = ct * c0 - st * s0
    sine = st * c0 + ct * s0
    sine = jnp.where(lane < head_size // 2, -sine, sine)

    def rotated(x):
        return (x * cosine + pltpu.roll(x, head_size // 2, 1) * sine).astype(jnp.bfloat16)

    for load in loads[2:4]:
        load.wait()
    small[0] = k_ref[...].astype(jnp.float32)
    small[1] = v_ref[...].astype(jnp.float32)
    for h in range(kv_heads):
        at = 1 + h * 2 * units
        k = rotated(small[0, pl.ds(h, tokens, stride=kv_heads), :])
        gathered[me, at : at + units] = k.reshape(units, UNIT, head_size)
        v = small[1, pl.ds(h, tokens, stride=kv_heads), :].astype(jnp.bfloat16)
        gathered[me, at + units : at + 2 * units] = v.reshape(units, UNIT, head_size)
    own = jnp.full((UNIT, head_size), offset, jnp.float32)
    gathered[me, 0] = own.astype(jnp.bfloat16)

    def copy(slot, p, target, kind):
        blocks = 2 * units * per_piece
        first = 1 + p * blocks if p else 0
        part = gathered.at[slot, pl.ds(first, 1 + (p + 1) * blocks - first)]
        return pltpu.make_async_remote_copy(
            src_ref=part,
            dst_ref=part,
            send_sem=send_sem.at[kind, slot, p],
            recv_sem=recv_sem.at[slot, p],
            device_id={"ctx": target},
        )

    def arrived(slot, p):
        copy(slot, p, mate, 0).wait_recv()

    def share(slot, p):
        copy(slot, p, across, 1).start()
        copy(slot, p, mate, 2).start()

    pl.semaphore_wait(barrier, 2 + (z > 0).astype(jnp.int32) + (z < rows - 1).astype(jnp.int32))

    for p in range(PIECES):

        @pl.when(z > 0)
        def _():
            copy(me, p, below, 0).start()

        @pl.when(z < rows - 1)
        def _():
            copy(me, p, above, 3).start()

        share(me, p)

    loads[4].wait()
    wide[...] = q_ref[...].astype(jnp.float32)
    for h in range(heads):
        k, g = divmod(h, per_group)
        q = rotated(wide[pl.ds(h, tokens, stride=heads), :])
        for t in range(tiles):
            q_rot[k, t * lanes + g * tile : t * lanes + (g + 1) * tile] = q[t * tile : (t + 1) * tile]

    width = tiles * lanes
    m_ref[...] = jnp.full(m_ref.shape, -jnp.inf, jnp.float32)
    l_ref[...] = jnp.zeros(l_ref.shape, jnp.float32)
    acc_ref[...] = jnp.zeros(acc_ref.shape, jnp.float32)

    keys_tile = PLANE * tile
    key_row = lax.broadcasted_iota(jnp.int32, (keys_tile, lanes), 0)
    key_at = key_row % tile
    query_at = lax.broadcasted_iota(jnp.int32, (keys_tile, lanes), 1) % tile

    def attend_plane(row):
        first = row * PLANE

        def head(k):
            at = 1 + k * 2 * units
            theirs = gathered[pl.ds(first, PLANE), 0].astype(jnp.float32)
            theirs = jnp.concatenate([theirs[:, None]] * (tile // UNIT), 1)
            theirs = theirs.reshape(keys_tile, head_size)
            reach = key_at + (theirs > offset).astype(jnp.int32)
            allowed = reach <= query_at
            scores = []
            for t in range(tiles):
                keys = gathered[pl.ds(first, PLANE), pl.ds(at + 2 * t, 2)]
                keys = keys.reshape(keys_tile, head_size)
                s = lax.dot_general(
                    keys, q_rot[k, t * lanes :],
                    (((1,), (1,)), ((), ())), preferred_element_type=jnp.float32,
                )
                diagonal = jnp.where(allowed, s[:, :lanes], -jnp.inf)
                scores.append([diagonal] + [s[:, i * lanes : (i + 1) * lanes] for i in range(1, tiles - t)])
            old = m_ref[k]
            weights = [[] for _ in range(tiles)]
            shrinks = []
            for i in range(tiles):
                span = slice(i * lanes, (i + 1) * lanes)
                mine = [scores[t][i - t] for t in range(i + 1)]
                top = old[:, span]
                for s in mine:
                    top = jnp.maximum(top, jnp.max(s, axis=0, keepdims=True))
                shrink = jnp.exp2((old[:, span] - top) * factor)
                total = l_ref[k, :, span] * shrink
                for t in range(i + 1):
                    w = jnp.exp2((mine[t] - top) * factor)
                    total += jnp.sum(w, axis=0, keepdims=True)
                    weights[t].append(w.astype(jnp.bfloat16))
                m_ref[k, :, span] = top
                l_ref[k, :, span] = total
                shrinks.append(shrink)
            sums = [acc_ref[k, :, i * lanes : (i + 1) * lanes] * shrinks[i] for i in range(tiles)]
            for t in range(tiles):
                values = gathered[pl.ds(first, PLANE), pl.ds(at + units + 2 * t, 2)]
                values = values.reshape(keys_tile, head_size)
                w = jnp.concatenate(weights[t], 1)
                o = lax.dot_general(
                    values, w, (((0,), (0,)), ((), ())), preferred_element_type=jnp.float32
                )
                for i in range(t, tiles):
                    sums[i] += o[:, (i - t) * lanes : (i - t + 1) * lanes]
            for i in range(tiles):
                acc_ref[k, :, i * lanes : (i + 1) * lanes] = sums[i]

        for p in range(PIECES):
            for col in range(2):
                arrived(device(row, col, 1 - core), p)

            @pl.loop(0, per_piece)
            def _(i):
                head(p * per_piece + i)

    def either(step, do):
        @pl.when(z >= step)
        def _():
            do(z - step, False)

        @pl.when(z + step < rows)
        def _():
            do(z + step, True)

    def relay_column(step):
        for p in range(PIECES):

            def do(row, from_above):
                slot = device(row, column, core)
                arrived(slot, p)
                if from_above:

                    @pl.when(z > 0)
                    def _():
                        copy(slot, p, below, 0).start()
                else:

                    @pl.when(z < rows - 1)
                    def _():
                        copy(slot, p, above, 3).start()
                share(slot, p)

            either(step, do)

    def relay_across(row):
        for p in range(PIECES):
            slot = device(row, 1 - column, core)
            arrived(slot, p)
            copy(slot, p, mate, 2).start()

    def finish(row, from_above):
        relay_across(row)
        attend_plane(row)

    relay_column(1)
    relay_across(z)
    attend_plane(z)

    @pl.loop(1, rows)
    def _(step):
        @pl.when(step + 1 < rows)
        def _():
            relay_column(step + 1)

        either(step, finish)

    for k in range(kv_heads):
        o = (acc_ref[k] / l_ref[k]).T
        for t in range(tiles):
            for g in range(per_group):
                at = t * lanes + g * tile
                wide[pl.ds(t * tile * heads + k * per_group + g, tile, stride=heads), :] = o[at : at + tile]
    out_ref[...] = wide[...].astype(jnp.bfloat16)

    def sent(row, from_above):
        for p in range(PIECES):
            slot = device(row, column, core)
            if from_above:

                @pl.when(z > 0)
                def _():
                    copy(slot, p, below, 0).wait_send()
            else:

                @pl.when(z < rows - 1)
                def _():
                    copy(slot, p, above, 3).wait_send()
            copy(slot, p, across, 1).wait_send()
            copy(slot, p, mate, 2).wait_send()
            copy(device(row, 1 - column, core), p, mate, 2).wait_send()

    @pl.loop(1, rows)
    def _(step):
        either(step, sent)

    sent(z, False)
    for p in range(PIECES):

        @pl.when(z > 0)
        def _():
            copy(me, p, below, 0).wait_send()


def solution(mesh):
    n = mesh.shape["ctx"]

    def shards(queries, keys, values, positions):
        tokens, heads, head_size = queries.shape
        kv_heads = keys.shape[1]
        per_group = heads // kv_heads
        table = rotary_tables(tokens, head_size, n)
        tile = 2 * UNIT
        width = tokens * per_group
        blocks = 1 + 2 * (tokens // UNIT) * kv_heads
        vmem = pl.BlockSpec(memory_space=pltpu.VMEM)
        hbm = pl.BlockSpec(memory_space=pl.ANY)
        out = pl.pallas_call(
            functools.partial(attend, n, kv_heads, per_group, tokens),
            out_shape=jax.ShapeDtypeStruct((tokens * heads, head_size), jnp.bfloat16),
            in_specs=[hbm] * 5,
            out_specs=vmem,
            scratch_shapes=[
                pltpu.VMEM((n, blocks, UNIT, head_size), jnp.bfloat16),
                pltpu.VMEM((kv_heads, width, head_size), jnp.bfloat16),
                pltpu.VMEM((tokens * heads, head_size), jnp.float32),
                pltpu.VMEM((2, tokens * kv_heads, head_size), jnp.float32),
                pltpu.VMEM((kv_heads, 1, width), jnp.float32),
                pltpu.VMEM((kv_heads, 1, width), jnp.float32),
                pltpu.VMEM((kv_heads, head_size, width), jnp.float32),
                pltpu.SMEM((tokens,), jnp.int32),
                pltpu.VMEM((tokens * heads, head_size), jnp.bfloat16),
                pltpu.VMEM((tokens * kv_heads, head_size), jnp.bfloat16),
                pltpu.VMEM((tokens * kv_heads, head_size), jnp.bfloat16),
                pltpu.VMEM(table.shape, jnp.float32),
                pltpu.SemaphoreType.DMA((n, PIECES)),
                pltpu.SemaphoreType.DMA((4, n, PIECES)),
                pltpu.SemaphoreType.DMA((5,)),
            ],
            compiler_params=pltpu.CompilerParams(
                collective_id=0, has_side_effects=True, vmem_limit_bytes=67043328
            ),
        )(
            positions,
            queries.reshape(tokens * heads, head_size),
            keys.reshape(tokens * kv_heads, head_size),
            values.reshape(tokens * kv_heads, head_size),
            table,
        )
        return out.reshape(tokens, heads, head_size)

    placed = (
        P(("groups", "ctx"), None, None),
        P(("groups", "ctx"), None, None),
        P(("groups", "ctx"), None, None),
        P(("groups", "ctx")),
    )
    return jax.shard_map(
        shards,
        mesh=mesh,
        in_specs=placed,
        out_specs=P(("groups", "ctx"), None, None),
        check_vma=False,
    )
```

```python
import functools
import math

import jax
import jax.numpy as jnp
import numpy as np
from jax import lax
from jax.experimental import pallas as pl
from jax.experimental.pallas import tpu as pltpu
from jax.sharding import PartitionSpec as P

UNIT = 16
PIECES = 2
PLANE = 4


def rotary_tables(tokens, head_size, stride):
    half = head_size // 2
    inverse = 1000000.0 ** (-2.0 * np.arange(half) / head_size)
    angles = (stride * np.arange(tokens))[:, None] * inverse[None, :]
    wide = lambda x: np.concatenate([x, x], -1)
    return np.concatenate(
        [wide(np.cos(angles)), wide(np.sin(angles)), wide(np.tile(inverse, (8, 1)))]
    ).astype(np.float32)


def attend(
    n, kv_heads, per_group, tokens,
    place_hbm, q_hbm, k_hbm, v_hbm, table_hbm, out_ref,
    gathered, q_rot, wide, small, m_ref, l_ref, acc_ref,
    place_ref, q_ref, k_ref, v_ref, table_ref,
    recv_sem, send_sem, load_sem,
):
    loads = [
        pltpu.make_async_copy(src, dst, load_sem.at[i])
        for i, (src, dst) in enumerate(
            [(place_hbm, place_ref), (table_hbm, table_ref), (k_hbm, k_ref), (v_hbm, v_ref), (q_hbm, q_ref)]
        )
    ]
    for load in loads:
        load.start()
    head_size = q_ref.shape[-1]
    heads = kv_heads * per_group
    rows = n // PLANE
    me = lax.axis_index("ctx")
    core = me % 2
    column = me // 2 % 2
    z = me // PLANE
    units = tokens // UNIT
    tile = 2 * UNIT
    tiles = tokens // tile
    per_piece = kv_heads // PIECES
    lanes = per_group * tile
    factor = math.log2(math.e) / math.sqrt(head_size)

    def device(row, col, cr):
        return row * PLANE + col * 2 + cr

    barrier = pltpu.get_barrier_semaphore()
    across = device(z, 1 - column, core)
    mate = device(z, column, 1 - core)
    below = me - PLANE
    above = me + PLANE

    def greet(target):
        pl.semaphore_signal(barrier, inc=1, device_id={"ctx": target})

    greet(across)
    greet(mate)

    @pl.when(z > 0)
    def _():
        greet(below)

    @pl.when(z < rows - 1)
    def _():
        greet(above)

    for load in loads[:2]:
        load.wait()
    offset = place_ref[0].astype(jnp.float32)
    start = table_ref[2 * tokens : 2 * tokens + 8, :] * offset
    c0, s0 = jnp.cos(start)[:1], jnp.sin(start)[:1]
    ct, st = table_ref[:tokens, :], table_ref[tokens : 2 * tokens, :]
    lane = lax.broadcasted_iota(jnp.int32, (tokens, head_size), 1)
    cosine = ct * c0 - st * s0
    sine = st * c0 + ct * s0
    sine = jnp.where(lane < head_size // 2, -sine, sine)

    def rotated(x):
        return (x * cosine + pltpu.roll(x, head_size // 2, 1) * sine).astype(jnp.bfloat16)

    for load in loads[2:4]:
        load.wait()
    small[0] = k_ref[...].astype(jnp.float32)
    small[1] = v_ref[...].astype(jnp.float32)
    for h in range(kv_heads):
        at = 1 + h * 2 * units
        k = rotated(small[0, pl.ds(h, tokens, stride=kv_heads), :])
        gathered[me, at : at + units] = k.reshape(units, UNIT, head_size)
        v = small[1, pl.ds(h, tokens, stride=kv_heads), :].astype(jnp.bfloat16)
        gathered[me, at + units : at + 2 * units] = v.reshape(units, UNIT, head_size)
    own = jnp.full((UNIT, head_size), offset, jnp.float32)
    gathered[me, 0] = own.astype(jnp.bfloat16)

    def copy(slot, p, target, kind):
        blocks = 2 * units * per_piece
        first = 1 + p * blocks if p else 0
        part = gathered.at[slot, pl.ds(first, 1 + (p + 1) * blocks - first)]
        return pltpu.make_async_remote_copy(
            src_ref=part,
            dst_ref=part,
            send_sem=send_sem.at[kind, slot, p],
            recv_sem=recv_sem.at[slot, p],
            device_id={"ctx": target},
        )

    def arrived(slot, p):
        copy(slot, p, mate, 0).wait_recv()

    def share(slot, p):
        copy(slot, p, across, 1).start()
        copy(slot, p, mate, 2).start()

    pl.semaphore_wait(barrier, 2 + (z > 0).astype(jnp.int32) + (z < rows - 1).astype(jnp.int32))

    for p in range(PIECES):

        @pl.when(z > 0)
        def _():
            copy(me, p, below, 0).start()

        @pl.when(z < rows - 1)
        def _():
            copy(me, p, above, 3).start()

        share(me, p)

    loads[4].wait()
    wide[...] = q_ref[...].astype(jnp.float32)
    for h in range(heads):
        k, g = divmod(h, per_group)
        q = rotated(wide[pl.ds(h, tokens, stride=heads), :])
        for t in range(tiles):
            q_rot[k, t * lanes + g * tile : t * lanes + (g + 1) * tile] = q[t * tile : (t + 1) * tile]

    width = tiles * lanes
    m_ref[...] = jnp.full(m_ref.shape, -jnp.inf, jnp.float32)
    l_ref[...] = jnp.zeros(l_ref.shape, jnp.float32)
    acc_ref[...] = jnp.zeros(acc_ref.shape, jnp.float32)

    keys_tile = PLANE * tile
    key_row = lax.broadcasted_iota(jnp.int32, (keys_tile, lanes), 0)
    key_at = key_row % tile
    query_at = lax.broadcasted_iota(jnp.int32, (keys_tile, lanes), 1) % tile

    def attend_plane(row):
        first = row * PLANE

        def head(k):
            at = 1 + k * 2 * units
            theirs = gathered[pl.ds(first, PLANE), 0].astype(jnp.float32)
            theirs = jnp.concatenate([theirs[:, None]] * (tile // UNIT), 1)
            theirs = theirs.reshape(keys_tile, head_size)
            reach = key_at + (theirs > offset).astype(jnp.int32)
            allowed = reach <= query_at
            scores = []
            for t in range(tiles):
                keys = gathered[pl.ds(first, PLANE), pl.ds(at + 2 * t, 2)]
                keys = keys.reshape(keys_tile, head_size)
                s = lax.dot_general(
                    keys, q_rot[k, t * lanes :],
                    (((1,), (1,)), ((), ())), preferred_element_type=jnp.float32,
                )
                diagonal = jnp.where(allowed, s[:, :lanes], -jnp.inf)
                scores.append([diagonal] + [s[:, i * lanes : (i + 1) * lanes] for i in range(1, tiles - t)])
            old = m_ref[k]
            weights = [[] for _ in range(tiles)]
            shrinks = []
            for i in range(tiles):
                span = slice(i * lanes, (i + 1) * lanes)
                mine = [scores[t][i - t] for t in range(i + 1)]
                top = old[:, span]
                for s in mine:
                    top = jnp.maximum(top, jnp.max(s, axis=0, keepdims=True))
                shrink = jnp.exp2((old[:, span] - top) * factor)
                total = l_ref[k, :, span] * shrink
                for t in range(i + 1):
                    w = jnp.exp2((mine[t] - top) * factor)
                    total += jnp.sum(w, axis=0, keepdims=True)
                    weights[t].append(w.astype(jnp.bfloat16))
                m_ref[k, :, span] = top
                l_ref[k, :, span] = total
                shrinks.append(shrink)
            sums = [acc_ref[k, :, i * lanes : (i + 1) * lanes] * shrinks[i] for i in range(tiles)]
            for t in range(tiles):
                values = gathered[pl.ds(first, PLANE), pl.ds(at + units + 2 * t, 2)]
                values = values.reshape(keys_tile, head_size)
                w = jnp.concatenate(weights[t], 1)
                o = lax.dot_general(
                    values, w, (((0,), (0,)), ((), ())), preferred_element_type=jnp.float32
                )
                for i in range(t, tiles):
                    sums[i] += o[:, (i - t) * lanes : (i - t + 1) * lanes]
            for i in range(tiles):
                acc_ref[k, :, i * lanes : (i + 1) * lanes] = sums[i]

        for p in range(PIECES):
            for col in range(2):
                arrived(device(row, col, 1 - core), p)

            for i in range(per_piece):
                head(p * per_piece + i)

    def either(step, do):
        @pl.when(z >= step)
        def _():
            do(z - step, False)

        @pl.when(z + step < rows)
        def _():
            do(z + step, True)

    def relay_column(step):
        for p in range(PIECES):

            def do(row, from_above):
                slot = device(row, column, core)
                arrived(slot, p)
                if from_above:

                    @pl.when(z > 0)
                    def _():
                        copy(slot, p, below, 0).start()
                else:

                    @pl.when(z < rows - 1)
                    def _():
                        copy(slot, p, above, 3).start()
                share(slot, p)

            either(step, do)

    def relay_across(row):
        for p in range(PIECES):
            slot = device(row, 1 - column, core)
            arrived(slot, p)
            copy(slot, p, mate, 2).start()

    def finish(row, from_above):
        relay_across(row)
        attend_plane(row)

    relay_column(1)
    relay_across(z)
    attend_plane(z)

    @pl.loop(1, rows)
    def _(step):
        @pl.when(step + 1 < rows)
        def _():
            relay_column(step + 1)

        either(step, finish)

    for k in range(kv_heads):
        o = (acc_ref[k] / l_ref[k]).T
        for t in range(tiles):
            for g in range(per_group):
                at = t * lanes + g * tile
                wide[pl.ds(t * tile * heads + k * per_group + g, tile, stride=heads), :] = o[at : at + tile]
    out_ref[...] = wide[...].astype(jnp.bfloat16)

    def sent(row, from_above):
        for p in range(PIECES):
            slot = device(row, column, core)
            if from_above:

                @pl.when(z > 0)
                def _():
                    copy(slot, p, below, 0).wait_send()
            else:

                @pl.when(z < rows - 1)
                def _():
                    copy(slot, p, above, 3).wait_send()
            copy(slot, p, across, 1).wait_send()
            copy(slot, p, mate, 2).wait_send()
            copy(device(row, 1 - column, core), p, mate, 2).wait_send()

    @pl.loop(1, rows)
    def _(step):
        either(step, sent)

    sent(z, False)
    for p in range(PIECES):

        @pl.when(z > 0)
        def _():
            copy(me, p, below, 0).wait_send()


def solution(mesh):
    n = mesh.shape["ctx"]

    def shards(queries, keys, values, positions):
        tokens, heads, head_size = queries.shape
        kv_heads = keys.shape[1]
        per_group = heads // kv_heads
        table = rotary_tables(tokens, head_size, n)
        tile = 2 * UNIT
        width = tokens * per_group
        blocks = 1 + 2 * (tokens // UNIT) * kv_heads
        vmem = pl.BlockSpec(memory_space=pltpu.VMEM)
        hbm = pl.BlockSpec(memory_space=pl.ANY)
        out = pl.pallas_call(
            functools.partial(attend, n, kv_heads, per_group, tokens),
            out_shape=jax.ShapeDtypeStruct((tokens * heads, head_size), jnp.bfloat16),
            in_specs=[hbm] * 5,
            out_specs=vmem,
            scratch_shapes=[
                pltpu.VMEM((n, blocks, UNIT, head_size), jnp.bfloat16),
                pltpu.VMEM((kv_heads, width, head_size), jnp.bfloat16),
                pltpu.VMEM((tokens * heads, head_size), jnp.float32),
                pltpu.VMEM((2, tokens * kv_heads, head_size), jnp.float32),
                pltpu.VMEM((kv_heads, 1, width), jnp.float32),
                pltpu.VMEM((kv_heads, 1, width), jnp.float32),
                pltpu.VMEM((kv_heads, head_size, width), jnp.float32),
                pltpu.SMEM((tokens,), jnp.int32),
                pltpu.VMEM((tokens * heads, head_size), jnp.bfloat16),
                pltpu.VMEM((tokens * kv_heads, head_size), jnp.bfloat16),
                pltpu.VMEM((tokens * kv_heads, head_size), jnp.bfloat16),
                pltpu.VMEM(table.shape, jnp.float32),
                pltpu.SemaphoreType.DMA((n, PIECES)),
                pltpu.SemaphoreType.DMA((4, n, PIECES)),
                pltpu.SemaphoreType.DMA((5,)),
            ],
            compiler_params=pltpu.CompilerParams(
                collective_id=0, has_side_effects=True, vmem_limit_bytes=48*1024*1024
            ),
        )(
            *(
                pltpu.with_memory_space_constraint(x, pltpu.HBM)
                for x in (
                    positions,
                    queries.reshape(tokens * heads, head_size),
                    keys.reshape(tokens * kv_heads, head_size),
                    values.reshape(tokens * kv_heads, head_size),
                    jnp.asarray(table),
                )
            )
        )
        return out.reshape(tokens, heads, head_size)

    placed = (
        P(("groups", "ctx"), None, None),
        P(("groups", "ctx"), None, None),
        P(("groups", "ctx"), None, None),
        P(("groups", "ctx")),
    )
    return jax.shard_map(
        shards,
        mesh=mesh,
        in_specs=placed,
        out_specs=P(("groups", "ctx"), None, None),
        check_vma=False,
    )
```

```python
import functools
import math

import jax
import jax.numpy as jnp
import numpy as np
from jax import lax
from jax.experimental import pallas as pl
from jax.experimental.pallas import tpu as pltpu
from jax.sharding import PartitionSpec as P

UNIT = 16
PIECES = 2
PLANE = 4


def rotary_tables(tokens, head_size, stride):
    half = head_size // 2
    inverse = 1000000.0 ** (-2.0 * np.arange(half) / head_size)
    angles = (stride * np.arange(tokens))[:, None] * inverse[None, :]
    wide = lambda x: np.concatenate([x, x], -1)
    return np.concatenate(
        [wide(np.cos(angles)), wide(np.sin(angles)), wide(np.tile(inverse, (8, 1)))]
    ).astype(np.float32)


def attend(
    n, kv_heads, per_group, tokens,
    place_hbm, q_hbm, k_hbm, v_hbm, table_hbm, out_ref,
    gathered, q_rot, wide, small, m_ref, l_ref, acc_ref,
    place_ref, q_ref, k_ref, v_ref, table_ref,
    recv_sem, send_sem, load_sem,
):
    loads = [
        pltpu.make_async_copy(src, dst, load_sem.at[i])
        for i, (src, dst) in enumerate(
            [(place_hbm, place_ref), (table_hbm, table_ref), (k_hbm, k_ref), (v_hbm, v_ref), (q_hbm, q_ref)]
        )
    ]
    for load in loads[:4]:
        load.start()
    head_size = q_ref.shape[-1]
    heads = kv_heads * per_group
    rows = n // PLANE
    me = lax.axis_index("ctx")
    core = me % 2
    column = me // 2 % 2
    z = me // PLANE
    units = tokens // UNIT
    tile = 2 * UNIT
    tiles = tokens // tile
    per_piece = kv_heads // PIECES
    lanes = per_group * tile
    factor = math.log2(math.e) / math.sqrt(head_size)

    def device(row, col, cr):
        return row * PLANE + col * 2 + cr

    barrier = pltpu.get_barrier_semaphore()
    across = device(z, 1 - column, core)
    mate = device(z, column, 1 - core)
    below = me - PLANE
    above = me + PLANE

    def greet(target):
        pl.semaphore_signal(barrier, inc=1, device_id={"ctx": target})

    greet(across)
    greet(mate)

    @pl.when(z > 0)
    def _():
        greet(below)

    @pl.when(z < rows - 1)
    def _():
        greet(above)

    for load in loads[:2]:
        load.wait()
    offset = place_ref[0].astype(jnp.float32)
    start = table_ref[2 * tokens : 2 * tokens + 8, :] * offset
    c0, s0 = jnp.cos(start)[:1], jnp.sin(start)[:1]
    ct, st = table_ref[:tokens, :], table_ref[tokens : 2 * tokens, :]
    lane = lax.broadcasted_iota(jnp.int32, (tokens, head_size), 1)
    cosine = ct * c0 - st * s0
    sine = st * c0 + ct * s0
    sine = jnp.where(lane < head_size // 2, -sine, sine)

    def rotated(x):
        return (x * cosine + pltpu.roll(x, head_size // 2, 1) * sine).astype(jnp.bfloat16)

    for load in loads[2:4]:
        load.wait()
    loads[4].start()
    small[0] = k_ref[...].astype(jnp.float32)
    small[1] = v_ref[...].astype(jnp.float32)
    for h in range(kv_heads):
        at = 1 + h * 2 * units
        k = rotated(small[0, pl.ds(h, tokens, stride=kv_heads), :])
        gathered[me, at : at + units] = k.reshape(units, UNIT, head_size)
        v = small[1, pl.ds(h, tokens, stride=kv_heads), :].astype(jnp.bfloat16)
        gathered[me, at + units : at + 2 * units] = v.reshape(units, UNIT, head_size)
    own = jnp.full((UNIT, head_size), offset, jnp.float32)
    gathered[me, 0] = own.astype(jnp.bfloat16)

    def copy(slot, p, target, kind):
        blocks = 2 * units * per_piece
        first = 1 + p * blocks if p else 0
        part = gathered.at[slot, pl.ds(first, 1 + (p + 1) * blocks - first)]
        return pltpu.make_async_remote_copy(
            src_ref=part,
            dst_ref=part,
            send_sem=send_sem.at[kind, slot, p],
            recv_sem=recv_sem.at[slot, p],
            device_id={"ctx": target},
        )

    def arrived(slot, p):
        copy(slot, p, mate, 0).wait_recv()

    def share(slot, p):
        copy(slot, p, across, 1).start()
        copy(slot, p, mate, 2).start()

    pl.semaphore_wait(barrier, 2 + (z > 0).astype(jnp.int32) + (z < rows - 1).astype(jnp.int32))

    for p in range(PIECES):

        @pl.when(z > 0)
        def _():
            copy(me, p, below, 0).start()

        @pl.when(z < rows - 1)
        def _():
            copy(me, p, above, 3).start()

        share(me, p)

    loads[4].wait()
    wide[...] = q_ref[...].astype(jnp.float32)
    for h in range(heads):
        k, g = divmod(h, per_group)
        q = rotated(wide[pl.ds(h, tokens, stride=heads), :])
        for t in range(tiles):
            q_rot[k, t * lanes + g * tile : t * lanes + (g + 1) * tile] = q[t * tile : (t + 1) * tile]

    width = tiles * lanes
    m_ref[...] = jnp.full(m_ref.shape, -jnp.inf, jnp.float32)
    l_ref[...] = jnp.zeros(l_ref.shape, jnp.float32)
    acc_ref[...] = jnp.zeros(acc_ref.shape, jnp.float32)

    keys_tile = PLANE * tile
    key_row = lax.broadcasted_iota(jnp.int32, (keys_tile, lanes), 0)
    key_at = key_row % tile
    query_at = lax.broadcasted_iota(jnp.int32, (keys_tile, lanes), 1) % tile

    def attend_plane(row):
        first = row * PLANE

        def head(k):
            at = 1 + k * 2 * units
            theirs = gathered[pl.ds(first, PLANE), 0].astype(jnp.float32)
            theirs = jnp.concatenate([theirs[:, None]] * (tile // UNIT), 1)
            theirs = theirs.reshape(keys_tile, head_size)
            reach = key_at + (theirs > offset).astype(jnp.int32)
            allowed = reach <= query_at
            scores = []
            for t in range(tiles):
                keys = gathered[pl.ds(first, PLANE), pl.ds(at + 2 * t, 2)]
                keys = keys.reshape(keys_tile, head_size)
                s = lax.dot_general(
                    keys, q_rot[k, t * lanes :],
                    (((1,), (1,)), ((), ())), preferred_element_type=jnp.float32,
                )
                diagonal = jnp.where(allowed, s[:, :lanes], -jnp.inf)
                scores.append([diagonal] + [s[:, i * lanes : (i + 1) * lanes] for i in range(1, tiles - t)])
            old = m_ref[k]
            weights = [[] for _ in range(tiles)]
            shrinks = []
            for i in range(tiles):
                span = slice(i * lanes, (i + 1) * lanes)
                mine = [scores[t][i - t] for t in range(i + 1)]
                top = old[:, span]
                for s in mine:
                    top = jnp.maximum(top, jnp.max(s, axis=0, keepdims=True))
                shrink = jnp.exp2((old[:, span] - top) * factor)
                total = l_ref[k, :, span] * shrink
                for t in range(i + 1):
                    w = jnp.exp2((mine[t] - top) * factor)
                    total += jnp.sum(w, axis=0, keepdims=True)
                    weights[t].append(w.astype(jnp.bfloat16))
                m_ref[k, :, span] = top
                l_ref[k, :, span] = total
                shrinks.append(shrink)
            sums = [acc_ref[k, :, i * lanes : (i + 1) * lanes] * shrinks[i] for i in range(tiles)]
            for t in range(tiles):
                values = gathered[pl.ds(first, PLANE), pl.ds(at + units + 2 * t, 2)]
                values = values.reshape(keys_tile, head_size)
                w = jnp.concatenate(weights[t], 1)
                o = lax.dot_general(
                    values, w, (((0,), (0,)), ((), ())), preferred_element_type=jnp.float32
                )
                for i in range(t, tiles):
                    sums[i] += o[:, (i - t) * lanes : (i - t + 1) * lanes]
            for i in range(tiles):
                acc_ref[k, :, i * lanes : (i + 1) * lanes] = sums[i]

        for p in range(PIECES):
            for col in range(2):
                arrived(device(row, col, 1 - core), p)

            for i in range(per_piece):
                head(p * per_piece + i)

    def either(step, do):
        @pl.when(z >= step)
        def _():
            do(z - step, False)

        @pl.when(z + step < rows)
        def _():
            do(z + step, True)

    def relay_column(step):
        for p in range(PIECES):

            def do(row, from_above):
                slot = device(row, column, core)
                arrived(slot, p)
                if from_above:

                    @pl.when(z > 0)
                    def _():
                        copy(slot, p, below, 0).start()
                else:

                    @pl.when(z < rows - 1)
                    def _():
                        copy(slot, p, above, 3).start()
                share(slot, p)

            either(step, do)

    def relay_across(row):
        for p in range(PIECES):
            slot = device(row, 1 - column, core)
            arrived(slot, p)
            copy(slot, p, mate, 2).start()

    relay_column(1)
    relay_across(z)
    attend_plane(z)

    @pl.loop(1, rows)
    def _(step):
        @pl.when(step + 1 < rows)
        def _():
            relay_column(step + 1)

        either(step, lambda row, from_above: relay_across(row))
        either(step, lambda row, from_above: attend_plane(row))

    for k in range(kv_heads):
        o = (acc_ref[k] / l_ref[k]).T
        for t in range(tiles):
            for g in range(per_group):
                at = t * lanes + g * tile
                wide[pl.ds(t * tile * heads + k * per_group + g, tile, stride=heads), :] = o[at : at + tile]
    out_ref[...] = wide[...].astype(jnp.bfloat16)

    def sent(row, from_above):
        for p in range(PIECES):
            slot = device(row, column, core)
            if from_above:

                @pl.when(z > 0)
                def _():
                    copy(slot, p, below, 0).wait_send()
            else:

                @pl.when(z < rows - 1)
                def _():
                    copy(slot, p, above, 3).wait_send()
            copy(slot, p, across, 1).wait_send()
            copy(slot, p, mate, 2).wait_send()
            copy(device(row, 1 - column, core), p, mate, 2).wait_send()

    @pl.loop(1, rows)
    def _(step):
        either(step, sent)

    sent(z, False)
    for p in range(PIECES):

        @pl.when(z > 0)
        def _():
            copy(me, p, below, 0).wait_send()


def solution(mesh):
    n = mesh.shape["ctx"]

    def shards(queries, keys, values, positions):
        tokens, heads, head_size = queries.shape
        kv_heads = keys.shape[1]
        per_group = heads // kv_heads
        table = rotary_tables(tokens, head_size, n)
        tile = 2 * UNIT
        width = tokens * per_group
        blocks = 1 + 2 * (tokens // UNIT) * kv_heads
        vmem = pl.BlockSpec(memory_space=pltpu.VMEM)
        hbm = pl.BlockSpec(memory_space=pl.ANY)
        out = pl.pallas_call(
            functools.partial(attend, n, kv_heads, per_group, tokens),
            out_shape=jax.ShapeDtypeStruct((tokens * heads, head_size), jnp.bfloat16),
            in_specs=[hbm] * 5,
            out_specs=vmem,
            scratch_shapes=[
                pltpu.VMEM((n, blocks, UNIT, head_size), jnp.bfloat16),
                pltpu.VMEM((kv_heads, width, head_size), jnp.bfloat16),
                pltpu.VMEM((tokens * heads, head_size), jnp.float32),
                pltpu.VMEM((2, tokens * kv_heads, head_size), jnp.float32),
                pltpu.VMEM((kv_heads, 1, width), jnp.float32),
                pltpu.VMEM((kv_heads, 1, width), jnp.float32),
                pltpu.VMEM((kv_heads, head_size, width), jnp.float32),
                pltpu.SMEM((tokens,), jnp.int32),
                pltpu.VMEM((tokens * heads, head_size), jnp.bfloat16),
                pltpu.VMEM((tokens * kv_heads, head_size), jnp.bfloat16),
                pltpu.VMEM((tokens * kv_heads, head_size), jnp.bfloat16),
                pltpu.VMEM(table.shape, jnp.float32),
                pltpu.SemaphoreType.DMA((n, PIECES)),
                pltpu.SemaphoreType.DMA((4, n, PIECES)),
                pltpu.SemaphoreType.DMA((5,)),
            ],
            compiler_params=pltpu.CompilerParams(
                collective_id=0, has_side_effects=True, vmem_limit_bytes=48*1024*1024
            ),
        )(
            *(
                pltpu.with_memory_space_constraint(x, pltpu.HBM)
                for x in (
                    positions,
                    queries.reshape(tokens * heads, head_size),
                    keys.reshape(tokens * kv_heads, head_size),
                    values.reshape(tokens * kv_heads, head_size),
                    jnp.asarray(table),
                )
            )
        )
        return out.reshape(tokens, heads, head_size)

    placed = (
        P(("groups", "ctx"), None, None),
        P(("groups", "ctx"), None, None),
        P(("groups", "ctx"), None, None),
        P(("groups", "ctx")),
    )
    return jax.shard_map(
        shards,
        mesh=mesh,
        in_specs=placed,
        out_specs=P(("groups", "ctx"), None, None),
        check_vma=False,
    )
```

```python
import functools
import math

import jax
import jax.numpy as jnp
import numpy as np
from jax import lax
from jax.experimental import pallas as pl
from jax.experimental.pallas import tpu as pltpu
from jax.sharding import PartitionSpec as P

UNIT = 16
PIECES = 2
PLANE = 4


def rotary_tables(tokens, head_size, stride):
    half = head_size // 2
    inverse = 1000000.0 ** (-2.0 * np.arange(half) / head_size)
    angles = (stride * np.arange(tokens))[:, None] * inverse[None, :]
    wide = lambda x: np.concatenate([x, x], -1)
    return np.concatenate(
        [wide(np.cos(angles)), wide(np.sin(angles)), wide(np.tile(inverse, (8, 1)))]
    ).astype(np.float32)


def attend(
    n, kv_heads, per_group, tokens,
    place_hbm, q_hbm, k_hbm, v_hbm, table_hbm, out_ref,
    gathered, q_rot, wide, small, m_ref, l_ref, acc_ref,
    place_ref, q_ref, k_ref, v_ref, table_ref,
    recv_sem, send_sem, load_sem,
):
    loads = [
        pltpu.make_async_copy(src, dst, load_sem.at[i])
        for i, (src, dst) in enumerate(
            [(place_hbm, place_ref), (table_hbm, table_ref), (k_hbm, k_ref), (v_hbm, v_ref), (q_hbm, q_ref)]
        )
    ]
    head_size = q_ref.shape[-1]
    heads = kv_heads * per_group
    rows = n // PLANE
    me = lax.axis_index("ctx")
    core = me % 2
    column = me // 2 % 2
    z = me // PLANE
    units = tokens // UNIT
    tile = 2 * UNIT
    tiles = tokens // tile
    per_piece = kv_heads // PIECES
    lanes = per_group * tile
    factor = math.log2(math.e) / math.sqrt(head_size)

    def device(row, col, cr):
        return row * PLANE + col * 2 + cr

    barrier = pltpu.get_barrier_semaphore()
    across = device(z, 1 - column, core)
    mate = device(z, column, 1 - core)
    below = me - PLANE
    above = me + PLANE

    def greet(target):
        pl.semaphore_signal(barrier, inc=1, device_id={"ctx": target})

    greet(across)
    greet(mate)

    @pl.when(z > 0)
    def _():
        greet(below)

    @pl.when(z < rows - 1)
    def _():
        greet(above)

    for load in loads[:4]:
        load.start()

    for load in loads[:2]:
        load.wait()
    offset = place_ref[0].astype(jnp.float32)
    start = table_ref[2 * tokens : 2 * tokens + 8, :] * offset
    c0, s0 = jnp.cos(start)[:1], jnp.sin(start)[:1]
    ct, st = table_ref[:tokens, :], table_ref[tokens : 2 * tokens, :]
    lane = lax.broadcasted_iota(jnp.int32, (tokens, head_size), 1)
    cosine = ct * c0 - st * s0
    sine = st * c0 + ct * s0
    sine = jnp.where(lane < head_size // 2, -sine, sine)

    def rotated(x):
        return (x * cosine + pltpu.roll(x, head_size // 2, 1) * sine).astype(jnp.bfloat16)

    for load in loads[2:4]:
        load.wait()
    loads[4].start()
    small[0] = k_ref[...].astype(jnp.float32)
    small[1] = v_ref[...].astype(jnp.float32)
    for h in range(kv_heads):
        at = 1 + h * 2 * units
        k = rotated(small[0, pl.ds(h, tokens, stride=kv_heads), :])
        gathered[me, at : at + units] = k.reshape(units, UNIT, head_size)
        v = small[1, pl.ds(h, tokens, stride=kv_heads), :].astype(jnp.bfloat16)
        gathered[me, at + units : at + 2 * units] = v.reshape(units, UNIT, head_size)
    own = jnp.full((UNIT, head_size), offset, jnp.float32)
    gathered[me, 0] = own.astype(jnp.bfloat16)

    def copy(slot, p, target, kind):
        blocks = 2 * units * per_piece
        first = 1 + p * blocks if p else 0
        part = gathered.at[slot, pl.ds(first, 1 + (p + 1) * blocks - first)]
        return pltpu.make_async_remote_copy(
            src_ref=part,
            dst_ref=part,
            send_sem=send_sem.at[kind, slot, p],
            recv_sem=recv_sem.at[slot, p],
            device_id={"ctx": target},
        )

    def arrived(slot, p):
        copy(slot, p, mate, 0).wait_recv()

    def share(slot, p):
        copy(slot, p, across, 1).start()
        copy(slot, p, mate, 2).start()

    pl.semaphore_wait(barrier, 2 + (z > 0).astype(jnp.int32) + (z < rows - 1).astype(jnp.int32))

    for p in range(PIECES):
        share(me, p)

        @pl.when(z > 0)
        def _():
            copy(me, p, below, 0).start()

        @pl.when(z < rows - 1)
        def _():
            copy(me, p, above, 3).start()


    loads[4].wait()
    wide[...] = q_ref[...].astype(jnp.float32)
    for h in range(heads):
        k, g = divmod(h, per_group)
        q = rotated(wide[pl.ds(h, tokens, stride=heads), :])
        for t in range(tiles):
            q_rot[k, t * lanes + g * tile : t * lanes + (g + 1) * tile] = q[t * tile : (t + 1) * tile]

    width = tiles * lanes
    m_ref[...] = jnp.full(m_ref.shape, -jnp.inf, jnp.float32)
    l_ref[...] = jnp.zeros(l_ref.shape, jnp.float32)
    acc_ref[...] = jnp.zeros(acc_ref.shape, jnp.float32)

    keys_tile = PLANE * tile
    key_row = lax.broadcasted_iota(jnp.int32, (keys_tile, lanes), 0)
    key_at = key_row % tile
    query_at = lax.broadcasted_iota(jnp.int32, (keys_tile, lanes), 1) % tile

    def attend_plane(row):
        first = row * PLANE

        def head(k):
            at = 1 + k * 2 * units
            theirs = gathered[pl.ds(first, PLANE), 0].astype(jnp.float32)
            theirs = jnp.concatenate([theirs[:, None]] * (tile // UNIT), 1)
            theirs = theirs.reshape(keys_tile, head_size)
            reach = key_at + (theirs > offset).astype(jnp.int32)
            allowed = reach <= query_at
            scores = []
            for t in range(tiles):
                keys = gathered[pl.ds(first, PLANE), pl.ds(at + 2 * t, 2)]
                keys = keys.reshape(keys_tile, head_size)
                s = lax.dot_general(
                    keys, q_rot[k, t * lanes :],
                    (((1,), (1,)), ((), ())), preferred_element_type=jnp.float32,
                )
                diagonal = jnp.where(allowed, s[:, :lanes], -jnp.inf)
                scores.append([diagonal] + [s[:, i * lanes : (i + 1) * lanes] for i in range(1, tiles - t)])
            old = m_ref[k]
            weights = [[] for _ in range(tiles)]
            shrinks = []
            for i in range(tiles):
                span = slice(i * lanes, (i + 1) * lanes)
                mine = [scores[t][i - t] for t in range(i + 1)]
                top = old[:, span]
                for s in mine:
                    top = jnp.maximum(top, jnp.max(s, axis=0, keepdims=True))
                shrink = jnp.exp2((old[:, span] - top) * factor)
                total = l_ref[k, :, span] * shrink
                for t in range(i + 1):
                    w = jnp.exp2((mine[t] - top) * factor)
                    total += jnp.sum(w, axis=0, keepdims=True)
                    weights[t].append(w.astype(jnp.bfloat16))
                m_ref[k, :, span] = top
                l_ref[k, :, span] = total
                shrinks.append(shrink)
            sums = [acc_ref[k, :, i * lanes : (i + 1) * lanes] * shrinks[i] for i in range(tiles)]
            for t in range(tiles):
                values = gathered[pl.ds(first, PLANE), pl.ds(at + units + 2 * t, 2)]
                values = values.reshape(keys_tile, head_size)
                w = jnp.concatenate(weights[t], 1)
                o = lax.dot_general(
                    values, w, (((0,), (0,)), ((), ())), preferred_element_type=jnp.float32
                )
                for i in range(t, tiles):
                    sums[i] += o[:, (i - t) * lanes : (i - t + 1) * lanes]
            for i in range(tiles):
                acc_ref[k, :, i * lanes : (i + 1) * lanes] = sums[i]

        for p in range(PIECES):
            for col in range(2):
                arrived(device(row, col, 1 - core), p)

            for i in range(per_piece):
                head(p * per_piece + i)

    def either(step, do):
        @pl.when(z >= step)
        def _():
            do(z - step, False)

        @pl.when(z + step < rows)
        def _():
            do(z + step, True)

    def relay_column(step):
        for p in range(PIECES):

            def do(row, from_above):
                slot = device(row, column, core)
                arrived(slot, p)
                if from_above:

                    @pl.when(z > 0)
                    def _():
                        copy(slot, p, below, 0).start()
                else:

                    @pl.when(z < rows - 1)
                    def _():
                        copy(slot, p, above, 3).start()
                share(slot, p)

            either(step, do)

    def relay_across(row):
        for p in range(PIECES):
            slot = device(row, 1 - column, core)
            arrived(slot, p)
            copy(slot, p, mate, 2).start()

    relay_column(1)
    relay_across(z)
    attend_plane(z)

    @pl.loop(1, rows)
    def _(step):
        @pl.when(step + 1 < rows)
        def _():
            relay_column(step + 1)

        either(step, lambda row, from_above: relay_across(row))
        either(step, lambda row, from_above: attend_plane(row))

    for k in range(kv_heads):
        o = (acc_ref[k] / l_ref[k]).T
        for t in range(tiles):
            for g in range(per_group):
                at = t * lanes + g * tile
                wide[pl.ds(t * tile * heads + k * per_group + g, tile, stride=heads), :] = o[at : at + tile]
    out_ref[...] = wide[...].astype(jnp.bfloat16)

    def sent(row, from_above):
        for p in range(PIECES):
            slot = device(row, column, core)
            if from_above:

                @pl.when(z > 0)
                def _():
                    copy(slot, p, below, 0).wait_send()
            else:

                @pl.when(z < rows - 1)
                def _():
                    copy(slot, p, above, 3).wait_send()
            copy(slot, p, across, 1).wait_send()
            copy(slot, p, mate, 2).wait_send()
            copy(device(row, 1 - column, core), p, mate, 2).wait_send()

    @pl.loop(1, rows)
    def _(step):
        either(step, sent)

    sent(z, False)
    for p in range(PIECES):

        @pl.when(z > 0)
        def _():
            copy(me, p, below, 0).wait_send()


def solution(mesh):
    n = mesh.shape["ctx"]

    def shards(queries, keys, values, positions):
        tokens, heads, head_size = queries.shape
        kv_heads = keys.shape[1]
        per_group = heads // kv_heads
        table = rotary_tables(tokens, head_size, n)
        tile = 2 * UNIT
        width = tokens * per_group
        blocks = 1 + 2 * (tokens // UNIT) * kv_heads
        vmem = pl.BlockSpec(memory_space=pltpu.VMEM)
        hbm = pl.BlockSpec(memory_space=pl.ANY)
        out = pl.pallas_call(
            functools.partial(attend, n, kv_heads, per_group, tokens),
            out_shape=jax.ShapeDtypeStruct((tokens * heads, head_size), jnp.bfloat16),
            in_specs=[hbm] * 5,
            out_specs=vmem,
            scratch_shapes=[
                pltpu.VMEM((n, blocks, UNIT, head_size), jnp.bfloat16),
                pltpu.VMEM((kv_heads, width, head_size), jnp.bfloat16),
                pltpu.VMEM((tokens * heads, head_size), jnp.float32),
                pltpu.VMEM((2, tokens * kv_heads, head_size), jnp.float32),
                pltpu.VMEM((kv_heads, 1, width), jnp.float32),
                pltpu.VMEM((kv_heads, 1, width), jnp.float32),
                pltpu.VMEM((kv_heads, head_size, width), jnp.float32),
                pltpu.SMEM((tokens,), jnp.int32),
                pltpu.VMEM((tokens * heads, head_size), jnp.bfloat16),
                pltpu.VMEM((tokens * kv_heads, head_size), jnp.bfloat16),
                pltpu.VMEM((tokens * kv_heads, head_size), jnp.bfloat16),
                pltpu.VMEM(table.shape, jnp.float32),
                pltpu.SemaphoreType.DMA((n, PIECES)),
                pltpu.SemaphoreType.DMA((4, n, PIECES)),
                pltpu.SemaphoreType.DMA((5,)),
            ],
            compiler_params=pltpu.CompilerParams(
                collective_id=0, has_side_effects=True, vmem_limit_bytes=48*1024*1024
            ),
        )(
            *(
                pltpu.with_memory_space_constraint(x, pltpu.HBM)
                for x in (
                    positions,
                    queries.reshape(tokens * heads, head_size),
                    keys.reshape(tokens * kv_heads, head_size),
                    values.reshape(tokens * kv_heads, head_size),
                    jnp.asarray(table),
                )
            )
        )
        return out.reshape(tokens, heads, head_size)

    placed = (
        P(("groups", "ctx"), None, None),
        P(("groups", "ctx"), None, None),
        P(("groups", "ctx"), None, None),
        P(("groups", "ctx")),
    )
    return jax.shard_map(
        shards,
        mesh=mesh,
        in_specs=placed,
        out_specs=P(("groups", "ctx"), None, None),
        check_vma=False,
    )
```
